32 devices in a mesh: grp: 2 (over core), dp: 4 (over z), seq: 4 (over y, x).
Axes of the slice: x: 2, y: 2, z: 4, core: 2. Of those that a mesh axis runs over, the one named last changes fastest.
Arguments:
- latents: bfloat16 [4, 512, 3072], P('dp', 'seq'), may hold values from -6 to 6
- attended: bfloat16 [4, 512, 1536], P('dp', 'seq'), may hold values from -6 to 6
- gating: float32 [4, 3072], P('dp'), may hold values from -4 to 4
- weights: bfloat16 [2, 3072, 1536], P('grp', ('dp', 'seq')), may hold values from -0.15625 to 0.15625
- critic_position: bfloat16 [512, 3072], P('seq'), may hold values from -6 to 6
- critic_gain: float32 [3072], replicated, may hold values from 0.1 to 1.9
- critic_head: float32 [1536], replicated, may hold values from -0.15625 to 0.15625
- token_order: int32 [512], replicated, may hold values from 0 to 511, as said below
Outputs:
- weight_grads: float32 [2, 3072, 1536], P('grp', ('dp', 'seq'))
The draws below stay inside these ranges and needn't reach their ends.
Inputs may be any that keep to these rules, and one draw needn't show every extreme that they name: token_order is a permutation of the 512 positions; of each aligned block of 128 entries, exactly 32 values fall in each aligned block of 128 values.
All inputs are finite; a program needn't handle non-finite values.
Results may differ from the reference program's by a relative error of at most 0.0029.
Values may be sent and summed in bfloat16 or wider, within the bound.
No kernel may reach another device: no remote copies, remote signals or barrier semaphores. Data moves between devices by JAX's collectives and lax.ppermute only.
A program may use at most 64 MiB of HBM per device.

```python
from functools import partial
import jax
import jax.numpy as jnp
from jax import lax

D = 3072
HD = 1536
TOK = 128
CLIPS = 4
L = 512
SHARE = 32


def draw_token_order(key, part):
    seq_count = TOK // SHARE
    key_one, key_two = jax.random.split(key)

    def shuffle_one(subkey):
        return jax.random.permutation(subkey, TOK).astype(jnp.int32)
    local_orders = jax.vmap(shuffle_one)(jax.random.split(key_one, seq_count))
    grouped = local_orders.reshape(seq_count, seq_count, SHARE) + (jnp.arange(seq_count, dtype=jnp.int32) * TOK)[:, None, None]
    arriving = jnp.transpose(grouped, (1, 0, 2)).reshape(seq_count, TOK)
    shuffles = jax.vmap(shuffle_one)(jax.random.split(key_two, seq_count))
    placed = jnp.take_along_axis(arriving, shuffles, axis=1)
    return placed.reshape(L).astype(jnp.int32)


def level_of(stream_key, extent, cuts, smallest, top_value):
    loudness, own = 1.0, jax.random.fold_in(stream_key, 6)
    for position, parts in cuts:
        heights = jnp.exp(jax.random.uniform(jax.random.fold_in(own, position), (parts,), jnp.float32, smallest / len(cuts), top_value / len(cuts)))
        loudness = loudness * jnp.repeat(heights, extent[position] // parts).reshape([-1 if axis == position else 1 for axis in range(len(extent))])
    return loudness


def noise(key, extent, deviation, bound, cuts=(), kind=jnp.bfloat16):
    entries = deviation * jax.random.normal(key, extent, jnp.float32)
    if cuts:
        entries = entries * level_of(key, extent, cuts, -0.22, 0.18)
    return jnp.clip(entries, -bound, bound).astype(kind)


def setup_inputs(seed: int = 0) -> dict:
    seeds = jax.random.split(jax.random.key(seed), 9)
    latents = noise(seeds[0], (CLIPS, L, D), 1.0, 6.0, ((0, 4), (1, 4)))
    attended = noise(seeds[1], (CLIPS, L, HD), 1.0, 6.0, ((0, 4), (1, 4)))
    gating = noise(seeds[2], (CLIPS, D), 1.0, 4.0, ((0, 4),), jnp.float32)
    weights = noise(seeds[3], (2, D, HD), HD ** -0.5, 0.15625, ((0, 2), (1, 16)))
    critic_position = noise(seeds[4], (L, D), 1.0, 6.0, ((0, 4),))
    critic_gain = jnp.clip(1.0 + 0.18 * jax.random.normal(seeds[5], (D,), jnp.float32), 0.1, 1.9)
    critic_head = noise(seeds[6], (HD,), HD ** -0.5, 0.15625, (), jnp.float32)
    token_order = draw_token_order(jax.random.fold_in(seeds[8], 71), 0)
    return dict(latents=latents, attended=attended, gating=gating, weights=weights, critic_position=critic_position, critic_gain=critic_gain, critic_head=critic_head, token_order=token_order)


def normalize(values, gain):
    factor = lax.rsqrt(lax.optimization_barrier(jnp.mean(values * values, axis=-1, keepdims=True)) + 1e-06)
    return values * factor * gain

def critic_score(hidden, head):
    return lax.optimization_barrier(jnp.sum(jax.nn.gelu(hidden, approximate=True) * head, axis=-1))

def reference(latents, attended, gating, weights, critic_position, critic_gain, critic_head, token_order):
    flat_attended = attended.reshape(-1, attended.shape[-1])
    projected = jnp.dot(flat_attended, weights[0].T, preferred_element_type=jnp.float32).reshape(latents.shape)
    fake_clip = (latents.astype(jnp.float32) + gating[:, None, :] * projected).astype(jnp.bfloat16)
    critic_in = fake_clip[:, token_order, :].astype(jnp.float32) + critic_position.astype(jnp.float32)[None]
    normed, norm_back = jax.vjp(partial(normalize, gain=critic_gain), critic_in)
    normed_b = normed.astype(jnp.bfloat16)
    flat_normed = normed_b.reshape(-1, D)
    hidden = jnp.dot(flat_normed, weights[1], preferred_element_type=jnp.float32)
    scores, score_back = jax.vjp(partial(critic_score, head=critic_head), hidden)
    hidden_grad = score_back(-jax.nn.sigmoid(-scores))[0].astype(jnp.bfloat16)
    normed_grad = jnp.dot(hidden_grad, weights[1].T, preferred_element_type=jnp.float32).reshape(critic_in.shape)
    input_grad = norm_back(normed_grad)[0].astype(jnp.bfloat16)
    inverse = jnp.argsort(token_order).astype(jnp.int32)
    fake_grad = input_grad[:, inverse, :]
    projected_grad = (gating[:, None, :] * fake_grad.astype(jnp.float32)).astype(jnp.bfloat16)
    maker_grad = jnp.dot(projected_grad.reshape(-1, D).T, flat_attended, preferred_element_type=jnp.float32)
    critic_grad = jnp.dot(flat_normed.T, hidden_grad, preferred_element_type=jnp.float32)
    return jnp.stack([maker_grad, critic_grad])
```

```python
import jax
import jax.numpy as jnp
from jax import lax
from jax.sharding import PartitionSpec as P


def hop(block, axis, distance):
    route = [(i, i ^ distance) for i in range(lax.axis_size(axis))]
    return lax.ppermute(block, axis, route)


def part(array, axis, count, index):
    size = array.shape[axis] // count
    return lax.dynamic_slice_in_dim(array, index * size, size, axis)


def everyone(own, axis):
    return [own] + [hop(own, axis, k) for k in range(1, lax.axis_size(axis))]


def in_order(blocks, place):
    size = blocks[0].shape[0]
    whole = jnp.zeros((len(blocks) * size,) + blocks[0].shape[1:], blocks[0].dtype)
    for k, block in enumerate(blocks):
        whole = lax.dynamic_update_slice_in_dim(whole, block, (place ^ k) * size, 0)
    return whole


def shards(
    latents, attended, gating, weights, critic_position, critic_gain, critic_head, token_order
):
    bf16, f16, f32 = jnp.bfloat16, jnp.float16, jnp.float32
    length, model_width = latents.shape[1:]
    feature_width = attended.shape[2]
    dps, seqs, grps = lax.axis_size("dp"), lax.axis_size("seq"), lax.axis_size("grp")
    width = model_width // dps
    rows = length // grps
    grp, dp, seq = lax.axis_index("grp"), lax.axis_index("dp"), lax.axis_index("seq")
    first = grp == 0

    own_weight, other_weight = [], []
    for block in everyone(weights[0], "seq"):
        own_weight.append(block)
        other_weight.append(hop(block, "grp", 1))
    maker_weight = in_order(
        [jnp.where(first, a, b) for a, b in zip(own_weight, other_weight)], seq
    )
    critic_weight = in_order(
        [jnp.where(first, b, a) for a, b in zip(own_weight, other_weight)], seq
    )

    attended_own = part(attended[0], 0, grps, grp)
    latents_own = part(latents[0], 0, grps, grp)
    messages = [
        jnp.concatenate([attended_own, part(latents_own, 1, dps, dp ^ k)], axis=1)
        for k in range(dps)
    ]
    messages = [messages[0]] + [hop(messages[k], "dp", k) for k in range(1, dps)]
    attended_all = in_order([m[:, :feature_width] for m in messages], dp)
    latents_all = in_order([m[None, :, feature_width:] for m in messages], dp)
    gates = [part(gating, 1, dps, dp ^ k) for k in range(dps)]
    gates = in_order([gates[0]] + [hop(gates[k], "dp", k) for k in range(1, dps)], dp)
    gates = gates[:, None, :]

    columns = part(part(critic_position, 1, dps, dp), 1, grps, grp)
    column_rows = in_order(everyone(columns, "seq"), seq)
    wanted = seq * length + jnp.arange(length, dtype=jnp.int32)
    picks = (token_order[None, :] == wanted[:, None]).astype(bf16)
    placed = jnp.dot(picks, column_rows, preferred_element_type=f32).astype(bf16)
    mine = part(placed, 0, grps, grp)
    brought = hop(part(placed, 0, grps, 1 - grp), "grp", 1)
    position = jnp.concatenate(
        [jnp.where(first, mine, brought), jnp.where(first, brought, mine)], axis=1
    ).astype(f32)
    gain = part(critic_gain, 0, dps, dp)

    projected = jnp.einsum("th,dh->td", attended_all, maker_weight, preferred_element_type=f32)
    projected = projected.reshape(dps, rows, width)
    fake = (latents_all.astype(f32) + gates * projected).astype(bf16)

    critic_in = fake.astype(f32) + position[None]
    square_sum = sum(everyone(jnp.sum(critic_in * critic_in, axis=-1), "dp"))
    factor = lax.rsqrt(square_sum / model_width + 1e-06)[..., None]
    normed = (critic_in * factor * gain).astype(bf16).reshape(-1, width)
    partial = jnp.dot(normed, critic_weight, preferred_element_type=f32)
    hidden = part(partial, 0, dps, dp)
    for k in range(1, dps):
        hidden = hidden + hop(part(partial, 0, dps, dp ^ k).astype(f16), "dp", k).astype(f32)
    scores, slope_of = jax.vjp(
        lambda v: jnp.sum(jax.nn.gelu(v, approximate=True) * critic_head, axis=-1), hidden
    )
    hidden_grad = slope_of(-jax.nn.sigmoid(-scores))[0].astype(bf16)
    dots = jnp.sum(hidden_grad.astype(f32) * hidden, axis=-1, keepdims=True)
    high = lax.reduce_precision(dots, 8, 7)
    low = lax.reduce_precision(dots - high, 8, 7)
    lane = lax.broadcasted_iota(jnp.int32, (rows, 128), 1)
    tail = jnp.where(lane == 0, high, jnp.where(lane == 1, low, 0.0)).astype(bf16)
    gathered = lax.all_gather(
        jnp.concatenate([hidden_grad, tail], axis=1), "dp", axis=0, tiled=True
    )
    hidden_grads = gathered[:, :feature_width]
    tails = gathered[:, feature_width : feature_width + 2].astype(f32)
    dots_all = jnp.sum(tails, axis=-1).reshape(dps, rows, 1)
    normed_grad = jnp.einsum("th,dh->td", hidden_grads, critic_weight, preferred_element_type=f32)
    normed_grad = normed_grad.reshape(dps, rows, width)
    input_grad = gain * normed_grad * factor - critic_in * (
        factor * factor * dots_all / model_width
    )
    input_grad = input_grad.astype(bf16).astype(f32)
    maker_grad = (gates * input_grad).astype(bf16).reshape(-1, width)

    right_brought = hop(jnp.where(first, hidden_grads, attended_all), "grp", 1)
    left_brought = hop(jnp.where(first, normed, maker_grad), "grp", 1)
    left = jnp.concatenate([jnp.where(first, maker_grad, normed), left_brought], axis=0)
    right = jnp.concatenate([jnp.where(first, attended_all, hidden_grads), right_brought], axis=0)
    total = jnp.einsum("td,th->dh", left, right, preferred_element_type=f32)
    summed = part(total, 0, seqs, seq)
    for k in range(1, seqs):
        summed = summed + hop(part(total, 0, seqs, seq ^ k).astype(bf16), "seq", k).astype(f32)
    return summed[None]


def solution(mesh):
    return jax.shard_map(
        shards,
        mesh=mesh,
        in_specs=(
            P("dp", "seq", None),
            P("dp", "seq", None),
            P("dp", None),
            P("grp", ("dp", "seq"), None),
            P("seq", None),
            P(),
            P(),
            P(),
        ),
        out_specs=P("grp", ("dp", "seq"), None),
        check_vma=False,
    )
```

```python
import jax
import jax.numpy as jnp
from jax import lax
from jax.experimental import pallas as pl
from jax.experimental.pallas import tpu as pltpu
from jax.sharding import PartitionSpec as P


def hop(block, axis, distance):
    route = [(i, i ^ distance) for i in range(lax.axis_size(axis))]
    return lax.ppermute(block, axis, route)


def rounded(values):
    return lax.reduce_precision(values, 8, 7)


def part(array, axis, count, index):
    size = array.shape[axis] // count
    return lax.dynamic_slice_in_dim(array, index * size, size, axis)


def everyone(own, axis):
    return [own] + [hop(own, axis, k) for k in range(1, lax.axis_size(axis))]


def pieces(own, axis):
    count, rows = lax.axis_size(axis), own.shape[0]
    if count != 4 or rows % 32:
        return [((k, 0), block) for k, block in enumerate(everyone(own, axis))]
    near, side = hop(own, axis, 1), hop(own, axis, 2)
    half = rows // 2
    far_top = hop(near[:half], axis, 2)
    far_bottom = hop(side[half:], axis, 1)
    return [((0, 0), own), ((1, 0), near), ((2, 0), side), ((3, 0), far_top), ((3, half), far_bottom)]


def in_order(blocks, place, size, count):
    whole = jnp.zeros((count * size,) + blocks[0][1].shape[1:], blocks[0][1].dtype)
    for (k, row), block in blocks:
        whole = lax.dynamic_update_slice_in_dim(whole, block, (place ^ k) * size + row, 0)
    return whole


VMEM = pl.BlockSpec(memory_space=pltpu.VMEM)


def pack(attended, latents, gating, weight, positions, grps, dps):
    length, depth = attended.shape
    size = weight.shape[0]
    width, rows = latents.shape[1] // dps, length // grps
    half = width // grps
    strip = length * half // depth

    def kernel(attended_ref, latents_ref, gating_ref, weight_ref, positions_ref, *outs):
        grp, dp = lax.axis_index("grp"), lax.axis_index("dp")
        row = pl.ds(pl.multiple_of(grp * rows, 16), rows)
        for k in range(dps):
            column = pl.ds(pl.multiple_of((dp ^ k) * width, 128), width)
            outs[k][:, :depth] = attended_ref[row, :]
            outs[k][:, depth:] = latents_ref[row, column]
            outs[dps + k][...] = gating_ref[:, column]
        outs[-1][:size, :] = weight_ref[...]
        if size % 16 == 0:
            column = pl.ds(pl.multiple_of(dp * width + grp * half, 128), half)
            for i in range(length // strip):
                lines = positions_ref[i * strip : (i + 1) * strip, column]
                outs[-1][size:, i * half : (i + 1) * half] = lines

    bf16, f32 = jnp.bfloat16, jnp.float32
    packed = pl.pallas_call(
        kernel,
        out_shape=[jax.ShapeDtypeStruct((rows, depth + width), bf16)] * dps
        + [jax.ShapeDtypeStruct((1, width), f32)] * dps
        + [jax.ShapeDtypeStruct((size + strip, depth), bf16)],
        in_specs=[VMEM] * 5,
        out_specs=[VMEM] * (2 * dps + 1),
        name="pack",
    )(attended, latents, gating, weight, positions)
    return list(packed[:dps]), list(packed[dps:-1]), packed[-1]


def generate(aligned, messages, gates, position, gain, own_weight, twin_weight, spots, size):
    clips, parts = len(messages), len(spots)
    rows, width = position.shape
    depth = own_weight[0].shape[1]
    channels = width

    def kernel(*refs):
        message_refs, refs = refs[:clips], refs[clips:]
        gate_refs, refs = refs[:clips], refs[clips:]
        position_ref, gain_ref, refs = refs[0], refs[1], refs[2:]
        own_refs, twin_refs, refs = refs[:parts], refs[parts : 2 * parts], refs[2 * parts :]
        out_ref, critic_ref, tokens_ref, gates_ref, square_ref, *refs = refs
        block_refs, (maker_ref, high_ref, low_ref) = refs[:clips], refs[clips:]
        grp, dp = lax.axis_index("grp"), lax.axis_index("dp")
        seq = lax.axis_index("seq") if aligned else 0

        def fill(first_refs, second_refs):
            for i, (k, row) in enumerate(spots):
                count = min(size - row, own_refs[i].shape[0])
                here = pl.ds(pl.multiple_of((seq ^ k) * size + row, 16), count)
                maker_ref[here, :] = first_refs[i][:count, :]
                critic_ref[here, :] = second_refs[i][:count, :]

        @pl.when(grp == 0)
        def _():
            fill(own_refs, twin_refs)

        @pl.when(grp != 0)
        def _():
            fill(twin_refs, own_refs)

        for k in range(clips):
            here = pl.ds(pl.multiple_of((dp ^ k) * rows, 16), rows)
            tokens_ref[here, :] = message_refs[k][:rows, :depth]
        projected = lax.dot_general(
            tokens_ref[...],
            maker_ref[...],
            (((1,), (1,)), ((), ())),
            preferred_element_type=jnp.float32,
        )
        out_ref[...] = projected.reshape(clips, rows, channels)
        for k in range(clips):
            gate = gate_refs[k][...]
            gates_ref[dp ^ k] = gate
            latents = message_refs[k][:rows, depth:].astype(jnp.float32)
            fake = (latents + gate * out_ref[dp ^ k]).astype(jnp.bfloat16)
            values = fake.astype(jnp.float32) + position_ref[...]
            out_ref[dp ^ k] = values
            sums = values[:, :128] * values[:, :128]
            for i in range(128, channels, 128):
                sums = sums + values[:, i : i + 128] * values[:, i : i + 128]
            square_ref[dp ^ k] = jnp.sum(jnp.transpose(sums), axis=0, keepdims=True)
            mean = jnp.sum(sums, axis=1, keepdims=True) / channels
            scaled = values * lax.rsqrt(mean + 1e-06) * gain_ref[...]
            high = scaled.astype(jnp.bfloat16)
            high_ref[k * rows : (k + 1) * rows] = high
            low = scaled - high.astype(jnp.float32)
            low_ref[k * rows : (k + 1) * rows] = low.astype(jnp.bfloat16)
        partial = jnp.dot(high_ref[...], critic_ref[...], preferred_element_type=jnp.float32)
        partial = partial + jnp.dot(
            low_ref[...], critic_ref[...], preferred_element_type=jnp.float32
        )
        for k in range(clips):
            block_refs[k][...] = partial[k * rows : (k + 1) * rows].astype(block_refs[k].dtype)

    return pl.pallas_call(
        kernel,
        out_shape=[
            jax.ShapeDtypeStruct((clips, rows, channels), jnp.float32),
            jax.ShapeDtypeStruct((width, depth), jnp.bfloat16),
            jax.ShapeDtypeStruct((clips * rows, depth), jnp.bfloat16),
            jax.ShapeDtypeStruct((clips, 1, channels), jnp.float32),
            jax.ShapeDtypeStruct((clips, 1, rows), jnp.float32),
        ]
        + [jax.ShapeDtypeStruct((rows, depth), jnp.float32) for _ in range(clips)],
        in_specs=[VMEM] * (2 * clips + 2 + 2 * parts),
        out_specs=[VMEM] * (5 + clips),
        scratch_shapes=[
            pltpu.VMEM((width, depth), jnp.bfloat16),
            pltpu.VMEM((clips * rows, width), jnp.bfloat16),
            pltpu.VMEM((clips * rows, width), jnp.bfloat16),
        ],
        cost_estimate=pl.CostEstimate(
            flops=2 * clips * rows * depth * width,
            bytes_accessed=2 * depth * (width + clips * rows) + 8 * clips * rows * width,
            transcendentals=0,
        ),
        name="generate",
    )(*messages, *gates, position, gain[None, :], *own_weight, *twin_weight)


def shards(
    latents, attended, gating, weights, critic_position, critic_gain, critic_head, token_order
):
    bf16, f16, f32 = jnp.bfloat16, jnp.float16, jnp.float32
    length, model_width = latents.shape[1:]
    feature_width = attended.shape[2]
    dps, seqs, grps = lax.axis_size("dp"), lax.axis_size("seq"), lax.axis_size("grp")
    width = model_width // dps
    rows = length // grps
    grp, dp, seq = lax.axis_index("grp"), lax.axis_index("dp"), lax.axis_index("seq")
    first = grp == 0

    size = weights.shape[1]
    half = width // grps
    strip = length * half // feature_width

    messages, gates, own = pack(
        attended[0], latents[0], gating, weights[0], critic_position, grps, dps
    )
    messages = messages[:1] + [hop(messages[k], "dp", k) for k in range(1, dps)]
    gates = gates[:1] + [hop(gates[k], "dp", k) for k in range(1, dps)]

    if size % 16:
        columns = part(part(critic_position, 1, dps, dp), 1, grps, grp)
        lines = [columns[i : i + strip] for i in range(0, length, strip)]
        own = jnp.concatenate([weights[0], jnp.concatenate(lines, axis=1)], axis=0)
    found = pieces(own, "seq")
    if size % 16 == 0:
        spots, blocks = [spot for spot, _ in found], [block for _, block in found]
    else:
        whole = in_order([(spot, block[:size]) for spot, block in found], seq, size, seqs)
        spots, blocks = [(0, 0)], [whole]
    twins = [hop(block, "grp", 1) for block in blocks]

    column_rows = jnp.zeros((seqs * length, half), bf16)
    for (k, row), block in found:
        if row + block.shape[0] > size:
            lines = block[size - row :]
            lines = [lines[:, i : i + half] for i in range(0, feature_width, half)]
            column_rows = lax.dynamic_update_slice_in_dim(
                column_rows, jnp.concatenate(lines, axis=0), (seq ^ k) * length, 0
            )
    wanted = seq * length + jnp.arange(length, dtype=jnp.int32)
    picks = (token_order[None, :] == wanted[:, None]).astype(bf16)
    placed = jnp.dot(picks, column_rows, preferred_element_type=f32).astype(bf16)
    mine = part(placed, 0, grps, grp)
    brought = hop(part(placed, 0, grps, 1 - grp), "grp", 1)
    position = jnp.concatenate(
        [jnp.where(first, mine, brought), jnp.where(first, brought, mine)], axis=1
    ).astype(f32)
    gain = part(critic_gain, 0, dps, dp)

    critic_in, critic_weight, attended_all, gates, square, *terms = generate(
        size % 16 == 0,
        messages,
        gates,
        position,
        gain,
        blocks,
        twins,
        spots,
        size if size % 16 == 0 else width,
    )

    for k in range(1, dps):
        term = terms[k].astype(f16)
        terms[k] = hop(term, "dp", k)
    squares = everyone(square.reshape(dps, rows), "dp")
    factor = lax.rsqrt(sum(squares) / model_width + 1e-06)
    own_factor = part(factor, 0, dps, dp)
    hidden = sum(
        term.astype(f32)
        * (jnp.sqrt(part(block, 0, dps, dp) / width + 1e-06) * own_factor).reshape(rows, 1)
        for term, block in zip(terms, squares)
    )
    factor = factor[..., None]
    normed = (critic_in * factor * gain).astype(bf16).reshape(-1, width)
    scores, slope_of = jax.vjp(
        lambda v: jnp.sum(jax.nn.gelu(v, approximate=True) * critic_head, axis=-1), hidden
    )
    hidden_grad = slope_of(-jax.nn.sigmoid(-scores))[0].astype(bf16)
    dots = jnp.sum(hidden_grad.astype(f32) * hidden, axis=-1, keepdims=True)
    high = rounded(dots)
    low = rounded(dots - high)
    lane = lax.broadcasted_iota(jnp.int32, (rows, 128), 1)
    tail = jnp.where(lane == 0, high, jnp.where(lane == 1, low, 0.0)).astype(bf16)
    gathered = lax.all_gather(
        jnp.concatenate([hidden_grad, tail], axis=1), "dp", axis=0, tiled=True
    )
    hidden_grads = gathered[:, :feature_width]
    tails = gathered[:, feature_width : feature_width + 2].astype(f32)
    dots_all = jnp.sum(tails, axis=-1).reshape(dps, rows, 1)
    normed_grad = jnp.einsum("th,dh->td", hidden_grads, critic_weight, preferred_element_type=f32)
    normed_grad = normed_grad.reshape(dps, rows, width)
    input_grad = gain * normed_grad * factor - critic_in * (
        factor * factor * dots_all / model_width
    )
    maker_grad = (gates * rounded(input_grad)).astype(bf16).reshape(-1, width)

    right_brought = hop(jnp.where(first, hidden_grads, attended_all), "grp", 1)
    left_brought = hop(jnp.where(first, normed, maker_grad), "grp", 1)
    left = jnp.concatenate([jnp.where(first, maker_grad, normed), left_brought], axis=0)
    right = jnp.concatenate([jnp.where(first, attended_all, hidden_grads), right_brought], axis=0)
    total = jnp.einsum("td,th->dh", left, right, preferred_element_type=f32)
    blocks = [part(total, 0, seqs, seq ^ k) for k in range(seqs)]
    blocks = lax.optimization_barrier(blocks[:1] + [block.astype(bf16) for block in blocks[1:]])
    summed = blocks[0]
    for k in range(1, seqs):
        summed = summed + hop(blocks[k], "seq", k).astype(f32)
    return summed[None]


def solution(mesh):
    return jax.shard_map(
        shards,
        mesh=mesh,
        in_specs=(
            P("dp", "seq", None),
            P("dp", "seq", None),
            P("dp", None),
            P("grp", ("dp", "seq"), None),
            P("seq", None),
            P(),
            P(),
            P(),
        ),
        out_specs=P("grp", ("dp", "seq"), None),
        check_vma=False,
    )
```

```python
import jax
import jax.numpy as jnp
from jax import lax
from jax.experimental import pallas as pl
from jax.experimental.pallas import tpu as pltpu
from jax.sharding import PartitionSpec as P


def hop(block, axis, distance):
    route = [(i, i ^ distance) for i in range(lax.axis_size(axis))]
    return lax.ppermute(block, axis, route)


def rounded(values):
    return lax.reduce_precision(values, 8, 7)


def part(array, axis, count, index):
    size = array.shape[axis] // count
    return lax.dynamic_slice_in_dim(array, index * size, size, axis)


def everyone(own, axis):
    return [own] + [hop(own, axis, k) for k in range(1, lax.axis_size(axis))]


def pieces(own, axis):
    count, rows = lax.axis_size(axis), own.shape[0]
    if count != 4 or rows % 32:
        return [((k, 0), block) for k, block in enumerate(everyone(own, axis))]
    near, side = hop(own, axis, 1), hop(own, axis, 2)
    half = rows // 2
    far_top = hop(near[:half], axis, 2)
    far_bottom = hop(side[half:], axis, 1)
    return [((0, 0), own), ((1, 0), near), ((2, 0), side), ((3, 0), far_top), ((3, half), far_bottom)]


def in_order(blocks, place, size, count):
    whole = jnp.zeros((count * size,) + blocks[0][1].shape[1:], blocks[0][1].dtype)
    for (k, row), block in blocks:
        whole = lax.dynamic_update_slice_in_dim(whole, block, (place ^ k) * size + row, 0)
    return whole


VMEM = pl.BlockSpec(memory_space=pltpu.VMEM)


def pack(attended, latents, gating, weight, positions, grps, dps):
    length, depth = attended.shape
    size = weight.shape[0]
    width, rows = latents.shape[1] // dps, length // grps
    half = width // grps
    strip = length * half // depth

    def kernel(attended_ref, latents_ref, gating_ref, weight_ref, positions_ref, *outs):
        grp, dp = lax.axis_index("grp"), lax.axis_index("dp")
        row = pl.ds(pl.multiple_of(grp * rows, 16), rows)
        for k in range(dps):
            column = pl.ds(pl.multiple_of((dp ^ k) * width, 128), width)
            outs[k][:, :depth] = attended_ref[row, :]
            outs[k][:, depth:] = latents_ref[row, column]
            outs[dps + k][...] = gating_ref[:, column]
        outs[-1][:size, :] = weight_ref[...]
        if size % 16 == 0:
            column = pl.ds(pl.multiple_of(dp * width + grp * half, 128), half)
            for i in range(length // strip):
                lines = positions_ref[i * strip : (i + 1) * strip, column]
                outs[-1][size:, i * half : (i + 1) * half] = lines

    bf16, f32 = jnp.bfloat16, jnp.float32
    packed = pl.pallas_call(
        kernel,
        out_shape=[jax.ShapeDtypeStruct((rows, depth + width), bf16)] * dps
        + [jax.ShapeDtypeStruct((1, width), f32)] * dps
        + [jax.ShapeDtypeStruct((size + strip, depth), bf16)],
        in_specs=[VMEM] * 5,
        out_specs=[VMEM] * (2 * dps + 1),
        name="pack",
    )(attended, latents, gating, weight, positions)
    return list(packed[:dps]), list(packed[dps:-1]), packed[-1]


def generate(aligned, messages, gates, picks, gain, own_weight, twin_weight, spots, size, tables):
    clips, parts = len(messages), len(spots)
    rows, lines = picks.shape
    depth = own_weight[0].shape[1]
    channels = width = messages[0].shape[1] - depth
    half = width // 2

    def kernel(*refs):
        message_refs, refs = refs[:clips], refs[clips:]
        gate_refs, refs = refs[:clips], refs[clips:]
        picks_ref, gain_ref, refs = refs[0], refs[1], refs[2:]
        own_refs, twin_refs, refs = refs[:parts], refs[parts : 2 * parts], refs[2 * parts :]
        given_refs, refs = refs[: len(tables)], refs[len(tables) :]
        out_ref, critic_ref, tokens_ref, gates_ref, square_ref, *refs = refs
        block_refs, (maker_ref, high_ref, low_ref, table_ref) = refs[:clips], refs[clips:]
        grp, dp = lax.axis_index("grp"), lax.axis_index("dp")
        seq = lax.axis_index("seq") if aligned else 0

        def fill(first_refs, second_refs):
            for i, (k, row) in enumerate(spots):
                count = min(size - row, own_refs[i].shape[0])
                here = pl.ds(pl.multiple_of((seq ^ k) * size + row, 16), count)
                maker_ref[here, :] = first_refs[i][:count, :]
                critic_ref[here, :] = second_refs[i][:count, :]

        @pl.when(grp == 0)
        def _():
            fill(own_refs, twin_refs)

        @pl.when(grp != 0)
        def _():
            fill(twin_refs, own_refs)

        places = []
        for side, piece_refs in enumerate((own_refs, twin_refs)):
            if tables:
                table = given_refs[side][...]
            else:
                for i, (k, row) in enumerate(spots):
                    start, strip = size - row, piece_refs[i].shape[0] - size + row
                    for j in range(depth // half if strip > 0 else 0):
                        at = (k * (depth // half) + j) * strip
                        block = piece_refs[i][start:, j * half : (j + 1) * half]
                        table_ref[at : at + strip, :] = block
                table = table_ref[...]
            places.append(jnp.dot(picks_ref[...], table, preferred_element_type=jnp.float32))
        position = jnp.concatenate(
            [jnp.where(grp == 0, *places), jnp.where(grp == 0, *reversed(places))], axis=1
        )
        gain_row = gain_ref[:, pl.ds(pl.multiple_of(dp * width, 128), width)]
        for k in range(clips):
            here = pl.ds(pl.multiple_of((dp ^ k) * rows, 16), rows)
            tokens_ref[here, :] = message_refs[k][:rows, :depth]
        projected = lax.dot_general(
            tokens_ref[...],
            maker_ref[...],
            (((1,), (1,)), ((), ())),
            preferred_element_type=jnp.float32,
        )
        out_ref[...] = projected.reshape(clips, rows, channels)
        for k in range(clips):
            gate = gate_refs[k][...]
            gates_ref[dp ^ k] = gate
            latents = message_refs[k][:rows, depth:].astype(jnp.float32)
            fake = (latents + gate * out_ref[dp ^ k]).astype(jnp.bfloat16)
            values = fake.astype(jnp.float32) + position
            out_ref[dp ^ k] = values
            sums = values[:, :128] * values[:, :128]
            for i in range(128, channels, 128):
                sums = sums + values[:, i : i + 128] * values[:, i : i + 128]
            square_ref[dp ^ k] = jnp.sum(jnp.transpose(sums), axis=0, keepdims=True)
            mean = jnp.sum(sums, axis=1, keepdims=True) / channels
            scaled = values * lax.rsqrt(mean + 1e-06) * gain_row
            high = scaled.astype(jnp.bfloat16)
            high_ref[k * rows : (k + 1) * rows] = high
            low = scaled - high.astype(jnp.float32)
            low_ref[k * rows : (k + 1) * rows] = low.astype(jnp.bfloat16)
        partial = jnp.dot(high_ref[...], critic_ref[...], preferred_element_type=jnp.float32)
        partial = partial + jnp.dot(
            low_ref[...], critic_ref[...], preferred_element_type=jnp.float32
        )
        for k in range(clips):
            block_refs[k][...] = partial[k * rows : (k + 1) * rows].astype(block_refs[k].dtype)

    return pl.pallas_call(
        kernel,
        out_shape=[
            jax.ShapeDtypeStruct((clips, rows, channels), jnp.float32),
            jax.ShapeDtypeStruct((width, depth), jnp.bfloat16),
            jax.ShapeDtypeStruct((clips * rows, depth), jnp.bfloat16),
            jax.ShapeDtypeStruct((clips, 1, channels), jnp.float32),
            jax.ShapeDtypeStruct((clips, 1, rows), jnp.float32),
        ]
        + [jax.ShapeDtypeStruct((rows, depth), jnp.float32) for _ in range(clips)],
        in_specs=[VMEM] * (2 * clips + 2 + 2 * parts + len(tables)),
        out_specs=[VMEM] * (5 + clips),
        scratch_shapes=[
            pltpu.VMEM((width, depth), jnp.bfloat16),
            pltpu.VMEM((clips * rows, width), jnp.bfloat16),
            pltpu.VMEM((clips * rows, width), jnp.bfloat16),
            pltpu.VMEM((lines, half), jnp.bfloat16),
        ],
        cost_estimate=pl.CostEstimate(
            flops=2 * clips * rows * depth * width,
            bytes_accessed=2 * depth * (width + clips * rows) + 8 * clips * rows * width,
            transcendentals=0,
        ),
        name="generate",
    )(*messages, *gates, picks, gain[None, :], *own_weight, *twin_weight, *tables)


def shards(
    latents, attended, gating, weights, critic_position, critic_gain, critic_head, token_order
):
    bf16, f16, f32 = jnp.bfloat16, jnp.float16, jnp.float32
    length, model_width = latents.shape[1:]
    feature_width = attended.shape[2]
    dps, seqs, grps = lax.axis_size("dp"), lax.axis_size("seq"), lax.axis_size("grp")
    width = model_width // dps
    rows = length // grps
    grp, dp, seq = lax.axis_index("grp"), lax.axis_index("dp"), lax.axis_index("seq")
    first = grp == 0

    size = weights.shape[1]
    half = width // grps
    strip = length * half // feature_width

    messages, gates, own = pack(
        attended[0], latents[0], gating, weights[0], critic_position, grps, dps
    )
    messages = messages[:1] + [hop(messages[k], "dp", k) for k in range(1, dps)]
    gates = gates[:1] + [hop(gates[k], "dp", k) for k in range(1, dps)]

    if size % 16:
        columns = part(part(critic_position, 1, dps, dp), 1, grps, grp)
        lines = [columns[i : i + strip] for i in range(0, length, strip)]
        own = jnp.concatenate([weights[0], jnp.concatenate(lines, axis=1)], axis=0)
    found = pieces(own, "seq")
    if size % 16 == 0:
        spots, blocks = [spot for spot, _ in found], [block for _, block in found]
    else:
        whole = in_order([(spot, block[:size]) for spot, block in found], seq, size, seqs)
        spots, blocks = [(0, 0)], [whole]
    twins = [hop(block, "grp", 1) for block in blocks]

    tables = []
    if size % 16:
        lines = [block[size - row :] for (_, row), block in found if row + block.shape[0] > size]
        table = jnp.concatenate(
            [line[:, i : i + half] for line in lines for i in range(0, feature_width, half)]
        )
        tables = [table, hop(table, "grp", 1)]
    order = jnp.concatenate([part(token_order, 0, seqs, seq ^ k) for k in range(seqs)])
    wanted = seq * length + grp * rows + jnp.arange(rows, dtype=jnp.int32)
    picks = (order[None, :] == wanted[:, None]).astype(bf16)
    gain = part(critic_gain, 0, dps, dp)

    critic_in, critic_weight, attended_all, gates, square, *terms = generate(
        size % 16 == 0,
        messages,
        gates,
        picks,
        critic_gain,
        blocks,
        twins,
        spots,
        size if size % 16 == 0 else width,
        tables,
    )

    for k in range(1, dps):
        term = terms[k].astype(f16)
        terms[k] = hop(term, "dp", k)
    squares = everyone(square.reshape(dps, rows), "dp")
    factor = lax.rsqrt(sum(squares) / model_width + 1e-06)
    own_factor = part(factor, 0, dps, dp)
    hidden = sum(
        term.astype(f32)
        * (jnp.sqrt(part(block, 0, dps, dp) / width + 1e-06) * own_factor).reshape(rows, 1)
        for term, block in zip(terms, squares)
    )
    factor = factor[..., None]
    normed = (critic_in * factor * gain).astype(bf16).reshape(-1, width)
    scores, slope_of = jax.vjp(
        lambda v: jnp.sum(jax.nn.gelu(v, approximate=True) * critic_head, axis=-1), hidden
    )
    hidden_grad = slope_of(-jax.nn.sigmoid(-scores))[0].astype(bf16)
    dots = jnp.sum(hidden_grad.astype(f32) * hidden, axis=-1, keepdims=True)
    high = rounded(dots)
    low = rounded(dots - high)
    lane = lax.broadcasted_iota(jnp.int32, (rows, 128), 1)
    tail = jnp.where(lane == 0, high, jnp.where(lane == 1, low, 0.0)).astype(bf16)
    gathered = lax.all_gather(
        jnp.concatenate([hidden_grad, tail], axis=1), "dp", axis=0, tiled=True
    )
    hidden_grads = gathered[:, :feature_width]
    tails = gathered[:, feature_width : feature_width + 2].astype(f32)
    dots_all = jnp.sum(tails, axis=-1).reshape(dps, rows, 1)
    normed_grad = jnp.einsum("th,dh->td", hidden_grads, critic_weight, preferred_element_type=f32)
    normed_grad = normed_grad.reshape(dps, rows, width)
    input_grad = gain * normed_grad * factor - critic_in * (
        factor * factor * dots_all / model_width
    )
    maker_grad = (gates * rounded(input_grad)).astype(bf16).reshape(-1, width)

    right_brought = hop(jnp.where(first, hidden_grads, attended_all), "grp", 1)
    left_brought = hop(jnp.where(first, normed, maker_grad), "grp", 1)
    left = jnp.concatenate([jnp.where(first, maker_grad, normed), left_brought], axis=0)
    right = jnp.concatenate([jnp.where(first, attended_all, hidden_grads), right_brought], axis=0)
    total = jnp.einsum("td,th->dh", left, right, preferred_element_type=f32)
    blocks = [part(total, 0, seqs, seq ^ k) for k in range(seqs)]
    blocks = lax.optimization_barrier(blocks[:1] + [block.astype(bf16) for block in blocks[1:]])
    summed = blocks[0]
    for k in range(1, seqs):
        summed = summed + hop(blocks[k], "seq", k).astype(f32)
    return summed[None]


def solution(mesh):
    return jax.shard_map(
        shards,
        mesh=mesh,
        in_specs=(
            P("dp", "seq", None),
            P("dp", "seq", None),
            P("dp", None),
            P("grp", ("dp", "seq"), None),
            P("seq", None),
            P(),
            P(),
            P(),
        ),
        out_specs=P("grp", ("dp", "seq"), None),
        check_vma=False,
    )
```

```python
import jax
import jax.numpy as jnp
from jax import lax
from jax.experimental import pallas as pl
from jax.experimental.pallas import tpu as pltpu
from jax.sharding import PartitionSpec as P


def hop(block, axis, distance):
    route = [(i, i ^ distance) for i in range(lax.axis_size(axis))]
    return lax.ppermute(block, axis, route)


def rounded(values):
    return lax.reduce_precision(values, 8, 7)


def part(array, axis, count, index):
    size = array.shape[axis] // count
    return lax.dynamic_slice_in_dim(array, index * size, size, axis)


def everyone(own, axis):
    return [own] + [hop(own, axis, k) for k in range(1, lax.axis_size(axis))]


def pieces(own, axis):
    count, rows = lax.axis_size(axis), own.shape[0]
    if count != 4 or rows % 32:
        return [((k, 0), block) for k, block in enumerate(everyone(own, axis))]
    near, side = hop(own, axis, 1), hop(own, axis, 2)
    half = rows // 2
    far_top = hop(near[:half], axis, 2)
    far_bottom = hop(side[half:], axis, 1)
    return [((0, 0), own), ((1, 0), near), ((2, 0), side), ((3, 0), far_top), ((3, half), far_bottom)]


def in_order(blocks, place, size, count):
    whole = jnp.zeros((count * size,) + blocks[0][1].shape[1:], blocks[0][1].dtype)
    for (k, row), block in blocks:
        whole = lax.dynamic_update_slice_in_dim(whole, block, (place ^ k) * size + row, 0)
    return whole


VMEM = pl.BlockSpec(memory_space=pltpu.VMEM)


def pack(attended, latents, gating, weight, positions, grps, dps):
    length, depth = attended.shape
    size = weight.shape[0]
    width, rows = latents.shape[1] // dps, length // grps
    half = width // grps
    strip = length * half // depth

    def kernel(attended_ref, latents_ref, gating_ref, weight_ref, positions_ref, *outs):
        grp, dp = lax.axis_index("grp"), lax.axis_index("dp")
        row = pl.ds(pl.multiple_of(grp * rows, 16), rows)
        for k in range(dps):
            column = pl.ds(pl.multiple_of((dp ^ k) * width, 128), width)
            outs[k][:, :depth] = attended_ref[row, :]
            outs[k][:, depth:] = latents_ref[row, column]
            outs[dps + k][...] = gating_ref[:, column]
        outs[-1][:size, :] = weight_ref[...]
        if size % 16 == 0:
            column = pl.ds(pl.multiple_of(dp * width + grp * half, 128), half)
            for i in range(length // strip):
                lines = positions_ref[i * strip : (i + 1) * strip, column]
                outs[-1][size:, i * half : (i + 1) * half] = lines

    bf16, f32 = jnp.bfloat16, jnp.float32
    packed = pl.pallas_call(
        kernel,
        out_shape=[jax.ShapeDtypeStruct((rows, depth + width), bf16)] * dps
        + [jax.ShapeDtypeStruct((1, width), f32)] * dps
        + [jax.ShapeDtypeStruct((size + strip, depth), bf16)],
        in_specs=[VMEM] * 5,
        out_specs=[VMEM] * (2 * dps + 1),
        name="pack",
    )(attended, latents, gating, weight, positions)
    return list(packed[:dps]), list(packed[dps:-1]), packed[-1]


def generate(aligned, messages, gates, picks, gain, own_weight, twin_weight, spots, size, tables):
    clips, parts = len(messages), len(spots)
    rows, lines = picks.shape
    depth = own_weight[0].shape[1]
    channels = width = messages[0].shape[1] - depth
    half = width // 2

    def kernel(*refs):
        message_refs, refs = refs[:clips], refs[clips:]
        gate_refs, refs = refs[:clips], refs[clips:]
        picks_ref, gain_ref, refs = refs[0], refs[1], refs[2:]
        own_refs, twin_refs, refs = refs[:parts], refs[parts : 2 * parts], refs[2 * parts :]
        given_refs, refs = refs[: len(tables)], refs[len(tables) :]
        out_ref, critic_ref, tokens_ref, gates_ref, square_ref, *refs = refs
        block_refs, (maker_ref, high_ref, low_ref, table_ref) = refs[:clips], refs[clips:]
        grp, dp = lax.axis_index("grp"), lax.axis_index("dp")
        seq = lax.axis_index("seq") if aligned else 0

        def fill(first_refs, second_refs):
            for i, (k, row) in enumerate(spots):
                count = min(size - row, own_refs[i].shape[0])
                here = pl.ds(pl.multiple_of((seq ^ k) * size + row, 16), count)
                maker_ref[here, :] = first_refs[i][:count, :]
                critic_ref[here, :] = second_refs[i][:count, :]

        @pl.when(grp == 0)
        def _():
            fill(own_refs, twin_refs)

        @pl.when(grp != 0)
        def _():
            fill(twin_refs, own_refs)

        places = []
        for side, piece_refs in enumerate((own_refs, twin_refs)):
            if tables:
                table = given_refs[side][...]
            else:
                for i, (k, row) in enumerate(spots):
                    start, strip = size - row, piece_refs[i].shape[0] - size + row
                    for j in range(depth // half if strip > 0 else 0):
                        at = (k * (depth // half) + j) * strip
                        block = piece_refs[i][start:, j * half : (j + 1) * half]
                        table_ref[at : at + strip, :] = block
                table = table_ref[...]
            places.append(jnp.dot(picks_ref[...], table, preferred_element_type=jnp.float32))
        position = jnp.concatenate(
            [jnp.where(grp == 0, *places), jnp.where(grp == 0, *reversed(places))], axis=1
        )
        gain_row = gain_ref[:, pl.ds(pl.multiple_of(dp * width, 128), width)]
        for k in range(clips):
            here = pl.ds(pl.multiple_of((dp ^ k) * rows, 16), rows)
            tokens_ref[here, :] = message_refs[k][:rows, :depth]
        projected = lax.dot_general(
            tokens_ref[...],
            maker_ref[...],
            (((1,), (1,)), ((), ())),
            preferred_element_type=jnp.float32,
        )
        out_ref[...] = projected.reshape(clips, rows, channels)
        for k in range(clips):
            gate = gate_refs[k][...]
            gates_ref[dp ^ k] = gate
            latents = message_refs[k][:rows, depth:].astype(jnp.float32)
            fake = (latents + gate * out_ref[dp ^ k]).astype(jnp.bfloat16)
            values = fake.astype(jnp.float32) + position
            out_ref[dp ^ k] = values
            sums = values[:, :128] * values[:, :128]
            for i in range(128, channels, 128):
                sums = sums + values[:, i : i + 128] * values[:, i : i + 128]
            square_ref[dp ^ k] = jnp.sum(jnp.transpose(sums), axis=0, keepdims=True)
            mean = jnp.sum(sums, axis=1, keepdims=True) / channels
            scaled = values * lax.rsqrt(mean + 1e-06) * gain_row
            high = scaled.astype(jnp.bfloat16)
            high_ref[k * rows : (k + 1) * rows] = high
            low = scaled - high.astype(jnp.float32)
            low_ref[k * rows : (k + 1) * rows] = low.astype(jnp.bfloat16)
        partial = jnp.dot(high_ref[...], critic_ref[...], preferred_element_type=jnp.float32)
        partial = partial + jnp.dot(
            low_ref[...], critic_ref[...], preferred_element_type=jnp.float32
        )
        for k in range(clips):
            block_refs[k][...] = partial[k * rows : (k + 1) * rows].astype(block_refs[k].dtype)

    return pl.pallas_call(
        kernel,
        out_shape=[
            jax.ShapeDtypeStruct((clips, rows, channels), jnp.float32),
            jax.ShapeDtypeStruct((width, depth), jnp.bfloat16),
            jax.ShapeDtypeStruct((clips * rows, depth), jnp.bfloat16),
            jax.ShapeDtypeStruct((clips, 1, channels), jnp.float32),
            jax.ShapeDtypeStruct((clips, 1, rows), jnp.float32),
        ]
        + [jax.ShapeDtypeStruct((rows, depth), jnp.float32) for _ in range(clips)],
        in_specs=[VMEM] * (2 * clips + 2 + 2 * parts + len(tables)),
        out_specs=[VMEM] * (5 + clips),
        scratch_shapes=[
            pltpu.VMEM((width, depth), jnp.bfloat16),
            pltpu.VMEM((clips * rows, width), jnp.bfloat16),
            pltpu.VMEM((clips * rows, width), jnp.bfloat16),
            pltpu.VMEM((lines, half), jnp.bfloat16),
        ],
        cost_estimate=pl.CostEstimate(
            flops=2 * clips * rows * depth * width,
            bytes_accessed=2 * depth * (width + clips * rows) + 8 * clips * rows * width,
            transcendentals=0,
        ),
        name="generate",
    )(*messages, *gates, picks, gain[None, :], *own_weight, *twin_weight, *tables)


def reduce_blocks(total, axis, place):
    bf16, f32 = jnp.bfloat16, jnp.float32
    count = lax.axis_size(axis)
    rows = total.shape[0] // count
    if count != 4 or rows % 32:
        blocks = [part(total, 0, count, place ^ k) for k in range(count)]
        blocks = lax.optimization_barrier(blocks[:1] + [block.astype(bf16) for block in blocks[1:]])
        got = [hop(blocks[k], axis, k).astype(f32) for k in range(1, count)]
        return sum(got, blocks[0])
    ways, half = ((1, 2), (2, 1)), rows // 2
    kept, sent = [], []
    for side, (one, two) in enumerate(ways):
        own, first, second, far = (
            part(total, 0, 2 * count, 2 * (place ^ k) + side) for k in (0, one, two, 3)
        )
        sent.append(jnp.concatenate([first.astype(bf16), far.astype(bf16)]))
        kept.append((own, second))
    kept, sent = lax.optimization_barrier((kept, sent))
    got = [hop(sent[i], axis, ways[i][0]) for i in (0, 1)]
    passed = [(kept[i][1] + got[i][half:].astype(f32)).astype(bf16) for i in (0, 1)]
    passed = lax.optimization_barrier(passed)
    last = [hop(passed[i], axis, ways[i][1]) for i in (0, 1)]
    return jnp.concatenate(
        [kept[i][0] + got[i][:half].astype(f32) + last[i].astype(f32) for i in (0, 1)]
    )


def shards(
    latents, attended, gating, weights, critic_position, critic_gain, critic_head, token_order
):
    bf16, f16, f32 = jnp.bfloat16, jnp.float16, jnp.float32
    length, model_width = latents.shape[1:]
    feature_width = attended.shape[2]
    dps, seqs, grps = lax.axis_size("dp"), lax.axis_size("seq"), lax.axis_size("grp")
    width = model_width // dps
    rows = length // grps
    grp, dp, seq = lax.axis_index("grp"), lax.axis_index("dp"), lax.axis_index("seq")
    first = grp == 0

    size = weights.shape[1]
    half = width // grps
    strip = length * half // feature_width

    messages, gates, own = pack(
        attended[0], latents[0], gating, weights[0], critic_position, grps, dps
    )
    messages = messages[:1] + [hop(messages[k], "dp", k) for k in range(1, dps)]
    gates = gates[:1] + [hop(gates[k], "dp", k) for k in range(1, dps)]

    if size % 16:
        columns = part(part(critic_position, 1, dps, dp), 1, grps, grp)
        lines = [columns[i : i + strip] for i in range(0, length, strip)]
        own = jnp.concatenate([weights[0], jnp.concatenate(lines, axis=1)], axis=0)
    found = pieces(own, "seq")
    if size % 16 == 0:
        spots, blocks = [spot for spot, _ in found], [block for _, block in found]
    else:
        whole = in_order([(spot, block[:size]) for spot, block in found], seq, size, seqs)
        spots, blocks = [(0, 0)], [whole]
    twins = [hop(block, "grp", 1) for block in blocks]

    tables = []
    if size % 16:
        lines = [block[size - row :] for (_, row), block in found if row + block.shape[0] > size]
        table = jnp.concatenate(
            [line[:, i : i + half] for line in lines for i in range(0, feature_width, half)]
        )
        tables = [table, hop(table, "grp", 1)]
    order = jnp.concatenate([part(token_order, 0, seqs, seq ^ k) for k in range(seqs)])
    wanted = seq * length + grp * rows + jnp.arange(rows, dtype=jnp.int32)
    picks = (order[None, :] == wanted[:, None]).astype(bf16)
    gain = part(critic_gain, 0, dps, dp)

    critic_in, critic_weight, attended_all, gates, square, *terms = generate(
        size % 16 == 0,
        messages,
        gates,
        picks,
        critic_gain,
        blocks,
        twins,
        spots,
        size if size % 16 == 0 else width,
        tables,
    )

    for k in range(1, dps):
        term = terms[k].astype(f16)
        terms[k] = hop(term, "dp", k)
    squares = everyone(square.reshape(dps, rows), "dp")
    factor = lax.rsqrt(sum(squares) / model_width + 1e-06)
    own_factor = part(factor, 0, dps, dp)
    hidden = sum(
        term.astype(f32)
        * (jnp.sqrt(part(block, 0, dps, dp) / width + 1e-06) * own_factor).reshape(rows, 1)
        for term, block in zip(terms, squares)
    )
    factor = factor[..., None]
    normed = (critic_in * factor * gain).astype(bf16).reshape(-1, width)
    scores, slope_of = jax.vjp(
        lambda v: jnp.sum(jax.nn.gelu(v, approximate=True) * critic_head, axis=-1), hidden
    )
    hidden_grad = slope_of(-jax.nn.sigmoid(-scores))[0].astype(bf16)
    dots = jnp.sum(hidden_grad.astype(f32) * hidden, axis=-1, keepdims=True)
    high = rounded(dots)
    low = rounded(dots - high)
    lane = lax.broadcasted_iota(jnp.int32, (rows, 128), 1)
    tail = jnp.where(lane == 0, high, jnp.where(lane == 1, low, 0.0)).astype(bf16)
    gathered = lax.all_gather(
        jnp.concatenate([hidden_grad, tail], axis=1), "dp", axis=0, tiled=True
    )
    hidden_grads = gathered[:, :feature_width]
    tails = gathered[:, feature_width : feature_width + 2].astype(f32)
    dots_all = jnp.sum(tails, axis=-1).reshape(dps, rows, 1)
    normed_grad = jnp.einsum("th,dh->td", hidden_grads, critic_weight, preferred_element_type=f32)
    normed_grad = normed_grad.reshape(dps, rows, width)
    input_grad = gain * normed_grad * factor - critic_in * (
        factor * factor * dots_all / model_width
    )
    maker_grad = (gates * rounded(input_grad)).astype(bf16).reshape(-1, width)

    right_brought = hop(jnp.where(first, hidden_grads, attended_all), "grp", 1)
    left_brought = hop(jnp.where(first, normed, maker_grad), "grp", 1)
    left = jnp.concatenate([jnp.where(first, maker_grad, normed), left_brought], axis=0)
    right = jnp.concatenate([jnp.where(first, attended_all, hidden_grads), right_brought], axis=0)
    total = jnp.einsum("td,th->dh", left, right, preferred_element_type=f32)
    return reduce_blocks(total, "seq", seq)[None]


def solution(mesh):
    return jax.shard_map(
        shards,
        mesh=mesh,
        in_specs=(
            P("dp", "seq", None),
            P("dp", "seq", None),
            P("dp", None),
            P("grp", ("dp", "seq"), None),
            P("seq", None),
            P(),
            P(),
            P(),
        ),
        out_specs=P("grp", ("dp", "seq"), None),
        check_vma=False,
    )
```

```python
import jax
import jax.numpy as jnp
from jax import lax
from jax.experimental import pallas as pl
from jax.experimental.pallas import tpu as pltpu
from jax.sharding import PartitionSpec as P


def hop(block, axis, distance):
    route = [(i, i ^ distance) for i in range(lax.axis_size(axis))]
    return lax.ppermute(block, axis, route)


def rounded(values):
    return lax.reduce_precision(values, 8, 7)


def part(array, axis, count, index):
    size = array.shape[axis] // count
    return lax.dynamic_slice_in_dim(array, index * size, size, axis)


def everyone(own, axis):
    return [own] + [hop(own, axis, k) for k in range(1, lax.axis_size(axis))]


def pieces(own, axis):
    count, rows = lax.axis_size(axis), own.shape[0]
    if count != 4 or rows % 32:
        return [((k, 0), block) for k, block in enumerate(everyone(own, axis))]
    near, side = hop(own, axis, 1), hop(own, axis, 2)
    half = rows // 2
    far_top = hop(near[:half], axis, 2)
    far_bottom = hop(side[half:], axis, 1)
    return [((0, 0), own), ((1, 0), near), ((2, 0), side), ((3, 0), far_top), ((3, half), far_bottom)]


def in_order(blocks, place, size, count):
    whole = jnp.zeros((count * size,) + blocks[0][1].shape[1:], blocks[0][1].dtype)
    for (k, row), block in blocks:
        whole = lax.dynamic_update_slice_in_dim(whole, block, (place ^ k) * size + row, 0)
    return whole


VMEM = pl.BlockSpec(memory_space=pltpu.VMEM)


def pack(attended, latents, gating, weight, positions, grps, dps):
    length, depth = attended.shape
    size = weight.shape[0]
    width, rows = latents.shape[1] // dps, length // grps
    half = width // grps
    strip = length * half // depth

    def kernel(attended_ref, latents_ref, gating_ref, weight_ref, positions_ref, *refs):
        outs, sems = refs[:-1], refs[-1]
        grp, dp = lax.axis_index("grp"), lax.axis_index("dp")
        row = pl.ds(pl.multiple_of(grp * rows, 16), rows)
        moves = [(weight_ref, outs[-1].at[:size])]
        if size % 16 == 0:
            column = pl.ds(pl.multiple_of(dp * width + grp * half, 128), half)
            for i in range(length // strip):
                lines = positions_ref.at[i * strip : (i + 1) * strip, column]
                moves.append((lines, outs[-1].at[size:, i * half : (i + 1) * half]))
        for k in range(dps):
            column = pl.ds(pl.multiple_of((dp ^ k) * width, 128), width)
            moves.append((attended_ref.at[row, :], outs[k].at[:, :depth]))
            moves.append((latents_ref.at[row, column], outs[k].at[:, depth:]))
            moves.append((gating_ref.at[:, column], outs[dps + k]))
        copies = [
            pltpu.make_async_copy(source, target, sems.at[i])
            for i, (source, target) in enumerate(moves)
        ]
        for copy in copies:
            copy.start()
        for copy in copies:
            copy.wait()

    bf16, f32 = jnp.bfloat16, jnp.float32
    packed = pl.pallas_call(
        kernel,
        out_shape=[jax.ShapeDtypeStruct((rows, depth + width), bf16)] * dps
        + [jax.ShapeDtypeStruct((1, width), f32)] * dps
        + [jax.ShapeDtypeStruct((size + strip, depth), bf16)],
        in_specs=[pl.BlockSpec(memory_space=pltpu.HBM)] * 5,
        out_specs=[VMEM] * (2 * dps + 1),
        scratch_shapes=[pltpu.SemaphoreType.DMA((3 * dps + 1 + length // strip,))],
        name="pack",
    )(attended, latents, gating, weight, positions)
    return list(packed[:dps]), list(packed[dps:-1]), packed[-1]


def generate(aligned, messages, gates, picks, gain, own_weight, twin_weight, spots, size, tables):
    clips, parts = len(messages), len(spots)
    rows, lines = picks.shape
    depth = own_weight[0].shape[1]
    channels = width = messages[0].shape[1] - depth
    half = width // 2

    def kernel(*refs):
        message_refs, refs = refs[:clips], refs[clips:]
        gate_refs, refs = refs[:clips], refs[clips:]
        picks_ref, gain_ref, refs = refs[0], refs[1], refs[2:]
        own_refs, twin_refs, refs = refs[:parts], refs[parts : 2 * parts], refs[2 * parts :]
        given_refs, refs = refs[: len(tables)], refs[len(tables) :]
        out_ref, critic_ref, tokens_ref, gates_ref, square_ref, *refs = refs
        block_refs, (maker_ref, terms_ref, table_ref) = refs[:clips], refs[clips:]
        grp, dp = lax.axis_index("grp"), lax.axis_index("dp")
        seq = lax.axis_index("seq") if aligned else 0

        def fill(first_refs, second_refs):
            for i, (k, row) in enumerate(spots):
                count = min(size - row, own_refs[i].shape[0])
                here = pl.ds(pl.multiple_of((seq ^ k) * size + row, 16), count)
                maker_ref[here, :] = first_refs[i][:count, :]
                critic_ref[here, :] = second_refs[i][:count, :]

        @pl.when(grp == 0)
        def _():
            fill(own_refs, twin_refs)

        @pl.when(grp != 0)
        def _():
            fill(twin_refs, own_refs)

        places = []
        for side, piece_refs in enumerate((own_refs, twin_refs)):
            if tables:
                table = given_refs[side][...]
            else:
                for i, (k, row) in enumerate(spots):
                    start, strip = size - row, piece_refs[i].shape[0] - size + row
                    for j in range(depth // half if strip > 0 else 0):
                        at = (k * (depth // half) + j) * strip
                        block = piece_refs[i][start:, j * half : (j + 1) * half]
                        table_ref[at : at + strip, :] = block
                table = table_ref[...]
            places.append(jnp.dot(picks_ref[...], table, preferred_element_type=jnp.float32))
        position = jnp.concatenate(
            [jnp.where(grp == 0, *places), jnp.where(grp == 0, *reversed(places))], axis=1
        )
        gain_row = gain_ref[:, pl.ds(pl.multiple_of(dp * width, 128), width)]
        for k in range(clips):
            here = pl.ds(pl.multiple_of((dp ^ k) * rows, 16), rows)
            tokens_ref[here, :] = message_refs[k][:rows, :depth]
        projected = lax.dot_general(
            tokens_ref[...],
            maker_ref[...],
            (((1,), (1,)), ((), ())),
            preferred_element_type=jnp.float32,
        )
        out_ref[...] = projected.reshape(clips, rows, channels)
        for k in range(clips):
            gate = gate_refs[k][...]
            gates_ref[dp ^ k] = gate
            latents = message_refs[k][:rows, depth:].astype(jnp.float32)
            fake = (latents + gate * out_ref[dp ^ k]).astype(jnp.bfloat16)
            values = fake.astype(jnp.float32) + position
            out_ref[dp ^ k] = values
            sums = values[:, :128] * values[:, :128]
            for i in range(128, channels, 128):
                sums = sums + values[:, i : i + 128] * values[:, i : i + 128]
            square_ref[dp ^ k] = jnp.sum(jnp.transpose(sums), axis=0, keepdims=True)
            mean = jnp.sum(sums, axis=1, keepdims=True) / channels
            scaled = values * lax.rsqrt(mean + 1e-06) * gain_row
            high = scaled.astype(jnp.bfloat16)
            terms_ref[k * rows : (k + 1) * rows] = high
            low = scaled - high.astype(jnp.float32)
            terms_ref[(clips + k) * rows : (clips + k + 1) * rows] = low.astype(jnp.bfloat16)
        both = jnp.dot(terms_ref[...], critic_ref[...], preferred_element_type=jnp.float32)
        partial = both[: clips * rows] + both[clips * rows :]
        for k in range(clips):
            block_refs[k][...] = partial[k * rows : (k + 1) * rows].astype(block_refs[k].dtype)

    return pl.pallas_call(
        kernel,
        out_shape=[
            jax.ShapeDtypeStruct((clips, rows, channels), jnp.float32),
            jax.ShapeDtypeStruct((width, depth), jnp.bfloat16),
            jax.ShapeDtypeStruct((clips * rows, depth), jnp.bfloat16),
            jax.ShapeDtypeStruct((clips, 1, channels), jnp.float32),
            jax.ShapeDtypeStruct((clips, 1, rows), jnp.float32),
        ]
        + [jax.ShapeDtypeStruct((rows, depth), jnp.float32) for _ in range(clips)],
        in_specs=[VMEM] * (2 * clips + 2 + 2 * parts + len(tables)),
        out_specs=[VMEM] * (5 + clips),
        scratch_shapes=[
            pltpu.VMEM((width, depth), jnp.bfloat16),
            pltpu.VMEM((2 * clips * rows, width), jnp.bfloat16),
            pltpu.VMEM((lines, half), jnp.bfloat16),
        ],
        cost_estimate=pl.CostEstimate(
            flops=2 * clips * rows * depth * width,
            bytes_accessed=2 * depth * (width + clips * rows) + 8 * clips * rows * width,
            transcendentals=0,
        ),
        compiler_params=pltpu.CompilerParams(vmem_limit_bytes=49 * 2**20),
        name="generate",
    )(*messages, *gates, picks, gain[None, :], *own_weight, *twin_weight, *tables)


def reduce_blocks(total, axis, place):
    bf16, f32 = jnp.bfloat16, jnp.float32
    count = lax.axis_size(axis)
    rows = total.shape[0] // count
    if count != 4 or rows % 32:
        blocks = [part(total, 0, count, place ^ k) for k in range(count)]
        blocks = lax.optimization_barrier(blocks[:1] + [block.astype(bf16) for block in blocks[1:]])
        got = [hop(blocks[k], axis, k).astype(f32) for k in range(1, count)]
        return sum(got, blocks[0])
    ways, half = ((1, 2), (2, 1)), rows // 2
    kept, sent = [], []
    for side, (one, two) in enumerate(ways):
        own, first, second, far = (
            part(total, 0, 2 * count, 2 * (place ^ k) + side) for k in (0, one, two, 3)
        )
        sent.append(jnp.concatenate([first.astype(bf16), far.astype(bf16)]))
        kept.append((own, second))
    kept, sent = lax.optimization_barrier((kept, sent))
    got = [hop(sent[i], axis, ways[i][0]) for i in (0, 1)]
    passed = [(kept[i][1] + got[i][half:].astype(f32)).astype(bf16) for i in (0, 1)]
    passed = lax.optimization_barrier(passed)
    last = [hop(passed[i], axis, ways[i][1]) for i in (0, 1)]
    return jnp.concatenate(
        [kept[i][0] + got[i][:half].astype(f32) + last[i].astype(f32) for i in (0, 1)]
    )


def shards(
    latents, attended, gating, weights, critic_position, critic_gain, critic_head, token_order
):
    bf16, f16, f32 = jnp.bfloat16, jnp.float16, jnp.float32
    length, model_width = latents.shape[1:]
    feature_width = attended.shape[2]
    dps, seqs, grps = lax.axis_size("dp"), lax.axis_size("seq"), lax.axis_size("grp")
    width = model_width // dps
    rows = length // grps
    grp, dp, seq = lax.axis_index("grp"), lax.axis_index("dp"), lax.axis_index("seq")
    first = grp == 0

    size = weights.shape[1]
    half = width // grps
    strip = length * half // feature_width

    messages, gates, own = pack(
        attended[0], latents[0], gating, weights[0], critic_position, grps, dps
    )
    messages = messages[:1] + [hop(messages[k], "dp", k) for k in range(1, dps)]
    gates = gates[:1] + [hop(gates[k], "dp", k) for k in range(1, dps)]

    if size % 16:
        columns = part(part(critic_position, 1, dps, dp), 1, grps, grp)
        lines = [columns[i : i + strip] for i in range(0, length, strip)]
        own = jnp.concatenate([weights[0], jnp.concatenate(lines, axis=1)], axis=0)
    found = pieces(own, "seq")
    if size % 16 == 0:
        spots, blocks = [spot for spot, _ in found], [block for _, block in found]
    else:
        whole = in_order([(spot, block[:size]) for spot, block in found], seq, size, seqs)
        spots, blocks = [(0, 0)], [whole]
    twins = [hop(block, "grp", 1) for block in blocks]

    tables = []
    if size % 16:
        lines = [block[size - row :] for (_, row), block in found if row + block.shape[0] > size]
        table = jnp.concatenate(
            [line[:, i : i + half] for line in lines for i in range(0, feature_width, half)]
        )
        tables = [table, hop(table, "grp", 1)]
    order = jnp.concatenate([part(token_order, 0, seqs, seq ^ k) for k in range(seqs)])
    wanted = seq * length + grp * rows + jnp.arange(rows, dtype=jnp.int32)
    picks = (order[None, :] == wanted[:, None]).astype(bf16)
    gain = part(critic_gain, 0, dps, dp)

    critic_in, critic_weight, attended_all, gates, square, *terms = generate(
        size % 16 == 0,
        messages,
        gates,
        picks,
        critic_gain,
        blocks,
        twins,
        spots,
        size if size % 16 == 0 else width,
        tables,
    )

    for k in range(1, dps):
        term = terms[k].astype(f16)
        terms[k] = hop(term, "dp", k)
    squares = everyone(square.reshape(dps, rows), "dp")
    factor = lax.rsqrt(sum(squares) / model_width + 1e-06)
    own_factor = part(factor, 0, dps, dp)
    hidden = sum(
        term.astype(f32)
        * (jnp.sqrt(part(block, 0, dps, dp) / width + 1e-06) * own_factor).reshape(rows, 1)
        for term, block in zip(terms, squares)
    )
    factor = factor[..., None]
    normed = (critic_in * factor * gain).astype(bf16).reshape(-1, width)
    scores, slope_of = jax.vjp(
        lambda v: jnp.sum(jax.nn.gelu(v, approximate=True) * critic_head, axis=-1), hidden
    )
    hidden_grad = slope_of(-jax.nn.sigmoid(-scores))[0].astype(bf16)
    dots = jnp.sum(hidden_grad.astype(f32) * hidden, axis=-1, keepdims=True)
    high = rounded(dots)
    low = rounded(dots - high)
    lane = lax.broadcasted_iota(jnp.int32, (rows, 128), 1)
    tail = jnp.where(lane == 0, high, jnp.where(lane == 1, low, 0.0)).astype(bf16)
    gathered = lax.all_gather(
        jnp.concatenate([hidden_grad, tail], axis=1), "dp", axis=0, tiled=True
    )
    hidden_grads = gathered[:, :feature_width]
    tails = gathered[:, feature_width : feature_width + 2].astype(f32)
    dots_all = jnp.sum(tails, axis=-1).reshape(dps, rows, 1)
    normed_grad = jnp.einsum("th,dh->td", hidden_grads, critic_weight, preferred_element_type=f32)
    normed_grad = normed_grad.reshape(dps, rows, width)
    input_grad = gain * normed_grad * factor - critic_in * (
        factor * factor * dots_all / model_width
    )
    maker_grad = (gates * rounded(input_grad)).astype(bf16).reshape(-1, width)

    right_brought = hop(jnp.where(first, hidden_grads, attended_all), "grp", 1)
    left_brought = hop(jnp.where(first, normed, maker_grad), "grp", 1)
    left = jnp.concatenate([jnp.where(first, maker_grad, normed), left_brought], axis=0)
    right = jnp.concatenate([jnp.where(first, attended_all, hidden_grads), right_brought], axis=0)
    total = jnp.einsum("td,th->dh", left, right, preferred_element_type=f32)
    return reduce_blocks(total, "seq", seq)[None]


def solution(mesh):
    return jax.shard_map(
        shards,
        mesh=mesh,
        in_specs=(
            P("dp", "seq", None),
            P("dp", "seq", None),
            P("dp", None),
            P("grp", ("dp", "seq"), None),
            P("seq", None),
            P(),
            P(),
            P(),
        ),
        out_specs=P("grp", ("dp", "seq"), None),
        check_vma=False,
    )
```

```python
import jax
import jax.numpy as jnp
from jax import lax
from jax.experimental import pallas as pl
from jax.experimental.pallas import tpu as pltpu
from jax.sharding import PartitionSpec as P


def hop(block, axis, distance):
    route = [(i, i ^ distance) for i in range(lax.axis_size(axis))]
    return lax.ppermute(block, axis, route)


def rounded(values):
    return lax.reduce_precision(values, 8, 7)


def part(array, axis, count, index):
    size = array.shape[axis] // count
    return lax.dynamic_slice_in_dim(array, index * size, size, axis)


def everyone(own, axis):
    return [own] + [hop(own, axis, k) for k in range(1, lax.axis_size(axis))]


def pieces(own, axis):
    count = lax.axis_size(axis)
    if count != 4 or len(own) != 2:
        whole = own[0] if len(own) == 1 else jnp.concatenate(own, axis=0)
        return [((k, 0), block) for k, block in enumerate(everyone(whole, axis))]
    top, bottom = own
    row = top.shape[0]
    near_top, side_bottom = hop(top, axis, 1), hop(bottom, axis, 2)
    near_bottom, side_top = hop(bottom, axis, 1), hop(top, axis, 2)
    far_top = hop(near_top, axis, 2)
    far_bottom = hop(side_bottom, axis, 1)
    tops = [top, near_top, side_top, far_top]
    bottoms = [bottom, near_bottom, side_bottom, far_bottom]
    return [
        ((k, first), block)
        for k in range(4)
        for first, block in ((0, tops[k]), (row, bottoms[k]))
    ]


def in_order(blocks, place, size, count):
    whole = jnp.zeros((count * size,) + blocks[0][1].shape[1:], blocks[0][1].dtype)
    for (k, row), block in blocks:
        whole = lax.dynamic_update_slice_in_dim(whole, block, (place ^ k) * size + row, 0)
    return whole


VMEM = pl.BlockSpec(memory_space=pltpu.VMEM)


def pack(attended, latents, gating, weight, positions, grps, dps):
    length, depth = attended.shape
    size = weight.shape[0]
    width, rows = latents.shape[1] // dps, length // grps
    half = width // grps
    strip = length * half // depth
    cut = (size + strip) // 2 if size % 16 == 0 else 0
    ends = [cut, size + strip - cut] if cut else []

    def kernel(attended_ref, latents_ref, gating_ref, weight_ref, positions_ref, *refs):
        outs, sems = refs[:-1], refs[-1]
        grp, dp = lax.axis_index("grp"), lax.axis_index("dp")
        row = pl.ds(pl.multiple_of(grp * rows, 16), rows)
        moves = []
        if size % 16 == 0:
            column = pl.ds(pl.multiple_of(dp * width + grp * half, 128), half)
            for i in range(length // strip):
                lines = positions_ref.at[i * strip : (i + 1) * strip, column]
                moves.append((lines, outs[-1].at[size - cut :, i * half : (i + 1) * half]))
            moves.append((weight_ref.at[:cut], outs[-2]))
            moves.append((weight_ref.at[cut:], outs[-1].at[: size - cut]))
        for k in range(dps):
            column = pl.ds(pl.multiple_of((dp ^ k) * width, 128), width)
            moves.append((attended_ref.at[row, :], outs[k].at[:, :depth]))
            moves.append((latents_ref.at[row, column], outs[k].at[:, depth:]))
            moves.append((gating_ref.at[:, column], outs[dps + k]))
        copies = [
            pltpu.make_async_copy(source, target, sems.at[i])
            for i, (source, target) in enumerate(moves)
        ]
        for copy in copies:
            copy.start()
        for copy in copies:
            copy.wait()

    bf16, f32 = jnp.bfloat16, jnp.float32
    packed = pl.pallas_call(
        kernel,
        out_shape=[jax.ShapeDtypeStruct((rows, depth + width), bf16)] * dps
        + [jax.ShapeDtypeStruct((1, width), f32)] * dps
        + [jax.ShapeDtypeStruct((end, depth), bf16) for end in ends],
        in_specs=[pl.BlockSpec(memory_space=pltpu.HBM)] * 5,
        out_specs=[VMEM] * (2 * dps + len(ends)),
        scratch_shapes=[pltpu.SemaphoreType.DMA((3 * dps + 2 + length // strip,))],
        name="pack",
    )(attended, latents, gating, weight, positions)
    return list(packed[:dps]), list(packed[dps : 2 * dps]), list(packed[2 * dps :])


def generate(aligned, messages, gates, picks, gain, own_weight, twin_weight, spots, size, tables):
    clips, parts = len(messages), len(spots)
    rows, lines = picks.shape
    depth = own_weight[0].shape[1]
    channels = width = messages[0].shape[1] - depth
    half = width // 2

    def kernel(*refs):
        message_refs, refs = refs[:clips], refs[clips:]
        gate_refs, refs = refs[:clips], refs[clips:]
        picks_ref, gain_ref, refs = refs[0], refs[1], refs[2:]
        own_refs, twin_refs, refs = refs[:parts], refs[parts : 2 * parts], refs[2 * parts :]
        given_refs, refs = refs[: len(tables)], refs[len(tables) :]
        out_ref, critic_ref, tokens_ref, gates_ref, square_ref, *refs = refs
        block_refs, (maker_ref, terms_ref, table_ref) = refs[:clips], refs[clips:]
        grp, dp = lax.axis_index("grp"), lax.axis_index("dp")
        seq = lax.axis_index("seq") if aligned else 0

        def fill(first_refs, second_refs):
            for i, (k, row) in enumerate(spots):
                count = min(size - row, own_refs[i].shape[0])
                here = pl.ds(pl.multiple_of((seq ^ k) * size + row, 16), count)
                maker_ref[here, :] = first_refs[i][:count, :]
                critic_ref[here, :] = second_refs[i][:count, :]

        @pl.when(grp == 0)
        def _():
            fill(own_refs, twin_refs)

        @pl.when(grp != 0)
        def _():
            fill(twin_refs, own_refs)

        places = []
        for side, piece_refs in enumerate((own_refs, twin_refs)):
            if tables:
                table = given_refs[side][...]
            else:
                for i, (k, row) in enumerate(spots):
                    start, strip = size - row, piece_refs[i].shape[0] - size + row
                    for j in range(depth // half if strip > 0 else 0):
                        at = (k * (depth // half) + j) * strip
                        block = piece_refs[i][start:, j * half : (j + 1) * half]
                        table_ref[at : at + strip, :] = block
                table = table_ref[...]
            places.append(jnp.dot(picks_ref[...], table, preferred_element_type=jnp.float32))
        position = jnp.concatenate(
            [jnp.where(grp == 0, *places), jnp.where(grp == 0, *reversed(places))], axis=1
        )
        gain_row = gain_ref[:, pl.ds(pl.multiple_of(dp * width, 128), width)]
        for k in range(clips):
            here = pl.ds(pl.multiple_of((dp ^ k) * rows, 16), rows)
            tokens_ref[here, :] = message_refs[k][:rows, :depth]
        projected = lax.dot_general(
            tokens_ref[...],
            maker_ref[...],
            (((1,), (1,)), ((), ())),
            preferred_element_type=jnp.float32,
        )
        out_ref[...] = projected.reshape(clips, rows, channels)
        for k in range(clips):
            gate = gate_refs[k][...]
            gates_ref[dp ^ k] = gate
            latents = message_refs[k][:rows, depth:].astype(jnp.float32)
            fake = (latents + gate * out_ref[dp ^ k]).astype(jnp.bfloat16)
            values = fake.astype(jnp.float32) + position
            out_ref[dp ^ k] = values
            sums = values[:, :128] * values[:, :128]
            for i in range(128, channels, 128):
                sums = sums + values[:, i : i + 128] * values[:, i : i + 128]
            square_ref[dp ^ k] = jnp.sum(jnp.transpose(sums), axis=0, keepdims=True)
            mean = jnp.sum(sums, axis=1, keepdims=True) / channels
            scaled = values * lax.rsqrt(mean + 1e-06) * gain_row
            high = scaled.astype(jnp.bfloat16)
            terms_ref[k * rows : (k + 1) * rows] = high
            low = scaled - high.astype(jnp.float32)
            terms_ref[(clips + k) * rows : (clips + k + 1) * rows] = low.astype(jnp.bfloat16)
        both = jnp.dot(terms_ref[...], critic_ref[...], preferred_element_type=jnp.float32)
        partial = both[: clips * rows] + both[clips * rows :]
        for k in range(clips):
            block_refs[k][...] = partial[k * rows : (k + 1) * rows].astype(block_refs[k].dtype)

    return pl.pallas_call(
        kernel,
        out_shape=[
            jax.ShapeDtypeStruct((clips, rows, channels), jnp.float32),
            jax.ShapeDtypeStruct((width, depth), jnp.bfloat16),
            jax.ShapeDtypeStruct((clips * rows, depth), jnp.bfloat16),
            jax.ShapeDtypeStruct((clips, 1, channels), jnp.float32),
            jax.ShapeDtypeStruct((clips, 1, rows), jnp.float32),
        ]
        + [jax.ShapeDtypeStruct((rows, depth), jnp.float32) for _ in range(clips)],
        in_specs=[VMEM] * (2 * clips + 2 + 2 * parts + len(tables)),
        out_specs=[VMEM] * (5 + clips),
        scratch_shapes=[
            pltpu.VMEM((width, depth), jnp.bfloat16),
            pltpu.VMEM((2 * clips * rows, width), jnp.bfloat16),
            pltpu.VMEM((lines, half), jnp.bfloat16),
        ],
        cost_estimate=pl.CostEstimate(
            flops=2 * clips * rows * depth * width,
            bytes_accessed=2 * depth * (width + clips * rows) + 8 * clips * rows * width,
            transcendentals=0,
        ),
        compiler_params=pltpu.CompilerParams(vmem_limit_bytes=55 * 2**20),
        name="generate",
    )(*messages, *gates, picks, gain[None, :], *own_weight, *twin_weight, *tables)


def reduce_blocks(total, axis, place):
    bf16, f32 = jnp.bfloat16, jnp.float32
    count = lax.axis_size(axis)
    rows = total.shape[0] // count
    if count != 4 or rows % 32:
        blocks = [part(total, 0, count, place ^ k) for k in range(count)]
        blocks = lax.optimization_barrier(blocks[:1] + [block.astype(bf16) for block in blocks[1:]])
        got = [hop(blocks[k], axis, k).astype(f32) for k in range(1, count)]
        return sum(got, blocks[0])
    ways, half = ((1, 2), (2, 1)), rows // 2
    kept, sent = [], []
    for side, (one, two) in enumerate(ways):
        own, first, second, far = (
            part(total, 0, 2 * count, 2 * (place ^ k) + side) for k in (0, one, two, 3)
        )
        sent.append(jnp.concatenate([first.astype(bf16), far.astype(bf16)]))
        kept.append((own, second))
    kept, sent = lax.optimization_barrier((kept, sent))
    got = [hop(sent[i], axis, ways[i][0]) for i in (0, 1)]
    passed = [(kept[i][1] + got[i][half:].astype(f32)).astype(bf16) for i in (0, 1)]
    passed = lax.optimization_barrier(passed)
    last = [hop(passed[i], axis, ways[i][1]) for i in (0, 1)]
    return jnp.concatenate(
        [kept[i][0] + got[i][:half].astype(f32) + last[i].astype(f32) for i in (0, 1)]
    )


def shards(
    latents, attended, gating, weights, critic_position, critic_gain, critic_head, token_order
):
    bf16, f16, f32 = jnp.bfloat16, jnp.float16, jnp.float32
    length, model_width = latents.shape[1:]
    feature_width = attended.shape[2]
    dps, seqs, grps = lax.axis_size("dp"), lax.axis_size("seq"), lax.axis_size("grp")
    width = model_width // dps
    rows = length // grps
    grp, dp, seq = lax.axis_index("grp"), lax.axis_index("dp"), lax.axis_index("seq")
    first = grp == 0

    size = weights.shape[1]
    half = width // grps
    strip = length * half // feature_width

    messages, gates, own = pack(
        attended[0], latents[0], gating, weights[0], critic_position, grps, dps
    )
    messages = messages[:1] + [hop(messages[k], "dp", k) for k in range(1, dps)]
    gates = gates[:1] + [hop(gates[k], "dp", k) for k in range(1, dps)]

    if size % 16:
        columns = part(part(critic_position, 1, dps, dp), 1, grps, grp)
        lines = [columns[i : i + strip] for i in range(0, length, strip)]
        own = [jnp.concatenate([weights[0], jnp.concatenate(lines, axis=1)], axis=0)]
    found = pieces(own, "seq")
    if size % 16 == 0:
        spots, blocks = [spot for spot, _ in found], [block for _, block in found]
    else:
        whole = in_order([(spot, block[:size]) for spot, block in found], seq, size, seqs)
        spots, blocks = [(0, 0)], [whole]
    twins = [hop(block, "grp", 1) for block in blocks]

    tables = []
    if size % 16:
        lines = [block[size - row :] for (_, row), block in found if row + block.shape[0] > size]
        table = jnp.concatenate(
            [line[:, i : i + half] for line in lines for i in range(0, feature_width, half)]
        )
        tables = [table, hop(table, "grp", 1)]
    order = jnp.concatenate([part(token_order, 0, seqs, seq ^ k) for k in range(seqs)])
    wanted = seq * length + grp * rows + jnp.arange(rows, dtype=jnp.int32)
    picks = (order[None, :] == wanted[:, None]).astype(bf16)
    gain = part(critic_gain, 0, dps, dp)

    critic_in, critic_weight, attended_all, gates, square, *terms = generate(
        size % 16 == 0,
        messages,
        gates,
        picks,
        critic_gain,
        blocks,
        twins,
        spots,
        size if size % 16 == 0 else width,
        tables,
    )

    for k in range(1, dps):
        term = terms[k].astype(f16)
        terms[k] = hop(term, "dp", k)
    squares = everyone(square.reshape(dps, rows), "dp")
    factor = lax.rsqrt(sum(squares) / model_width + 1e-06)
    own_factor = part(factor, 0, dps, dp)
    hidden = sum(
        term.astype(f32)
        * (jnp.sqrt(part(block, 0, dps, dp) / width + 1e-06) * own_factor).reshape(rows, 1)
        for term, block in zip(terms, squares)
    )
    factor = factor[..., None]
    normed = (critic_in * factor * gain).astype(bf16).reshape(-1, width)
    scores, slope_of = jax.vjp(
        lambda v: jnp.sum(jax.nn.gelu(v, approximate=True) * critic_head, axis=-1), hidden
    )
    hidden_grad = slope_of(-jax.nn.sigmoid(-scores))[0].astype(bf16)
    dots = jnp.sum(hidden_grad.astype(f32) * hidden, axis=-1, keepdims=True)
    high = rounded(dots)
    low = rounded(dots - high)
    lane = lax.broadcasted_iota(jnp.int32, (rows, 128), 1)
    tail = jnp.where(lane == 0, high, jnp.where(lane == 1, low, 0.0)).astype(bf16)
    gathered = lax.all_gather(
        jnp.concatenate([hidden_grad, tail], axis=1), "dp", axis=0, tiled=True
    )
    hidden_grads = gathered[:, :feature_width]
    tails = gathered[:, feature_width : feature_width + 2].astype(f32)
    dots_all = jnp.sum(tails, axis=-1).reshape(dps, rows, 1)
    normed_grad = jnp.einsum("th,dh->td", hidden_grads, critic_weight, preferred_element_type=f32)
    normed_grad = normed_grad.reshape(dps, rows, width)
    input_grad = gain * normed_grad * factor - critic_in * (
        factor * factor * dots_all / model_width
    )
    maker_grad = (gates * rounded(input_grad)).astype(bf16).reshape(-1, width)

    right_brought = hop(jnp.where(first, hidden_grads, attended_all), "grp", 1)
    left_brought = hop(jnp.where(first, normed, maker_grad), "grp", 1)
    left = jnp.concatenate([jnp.where(first, maker_grad, normed), left_brought], axis=0)
    right = jnp.concatenate([jnp.where(first, attended_all, hidden_grads), right_brought], axis=0)
    total = jnp.einsum("td,th->dh", left, right, preferred_element_type=f32)
    return reduce_blocks(total, "seq", seq)[None]


def solution(mesh):
    return jax.shard_map(
        shards,
        mesh=mesh,
        in_specs=(
            P("dp", "seq", None),
            P("dp", "seq", None),
            P("dp", None),
            P("grp", ("dp", "seq"), None),
            P("seq", None),
            P(),
            P(),
            P(),
        ),
        out_specs=P("grp", ("dp", "seq"), None),
        check_vma=False,
    )
```
